32 devices in a mesh: space: 8 (over z, y), tm: 4 (over x, core).
Axes of the slice: x: 2, y: 2, z: 4, core: 2. Of those that a mesh axis runs over, the one named last changes fastest.
Arguments:
- precip: float32 [512, 48, 2048], P('tm', 'space'), may hold values from 0.0001 to 0.01
Outputs:
- totals: float32 [48, 2048, 512], P(None, 'space', 'tm')
The draws below stay inside these ranges and needn't reach their ends.
All inputs are finite; a program needn't handle non-finite values.
Results may differ from the reference program's by a relative error of at most 0.00005.
Values sent between devices are 32-bit elements; how exact they have to be, the bound alone decides.
A program may use at most 64 MiB of HBM per device.

```python
import math
import jax
import jax.numpy as jnp

LON = 2048
DAYS = 512
LAT = 48


def steps_of(rng, dims, split, least, high):
    def one(position, blocks):
        steps = jax.random.uniform(jax.random.fold_in(jax.random.fold_in(rng, 6), position), (blocks,), jnp.float32, least / len(split), high / len(split))
        return jnp.repeat(jnp.exp(steps), dims[position] // blocks).reshape((-1,) + (1,) * (len(dims) - position - 1))

    factor_of = one(*split[0])
    for cut in split[1:]:
        factor_of = factor_of * one(*cut)
    return factor_of


def setup_inputs(seed: int = 0) -> dict:
    key_list = jax.random.split(jax.random.key(seed), 2)
    precip = jnp.clip(jnp.exp(math.log(0.01) - 4.6051702 * jax.random.uniform(key_list[0], (DAYS, LAT, LON), jnp.float32) ** steps_of(key_list[0], (DAYS, LAT, LON), ((0, 4), (1, 8)), -0.2, 0.2)), 0.0001, 0.01)
    return {"precip": precip}


def reference(precip):
    running = jnp.cumsum(precip, axis=0)
    return jnp.transpose(running, (1, 2, 0))
```

```python
import functools

import jax
import jax.numpy as jnp
from jax import lax
from jax.experimental import pallas as pl
from jax.experimental.pallas import tpu as pltpu
from jax.sharding import PartitionSpec as P

MESH = pl.DeviceIdType.MESH
HEAD = 8
FIRST = 4
ROW = 2
INNER = {8: ((6, 5, 1, 2, 3, 4, 7), (6, 1, 2, 3, 5, 4, 7))}
OUTER = {8: ((2, 3, 1, 7, 6, 5, 4), (2, 1, 3, 7, 6, 5, 4))}
PARTS = (3, 2, 1)


def parts_of(lat):
    total = sum(PARTS)
    if lat % total:
        return ((0, lat),)
    unit, at, found = lat // total, 0, []
    for part in PARTS:
        found.append((at, part * unit))
        at += part * unit
    return tuple(found)


def flip(place, mask, size):
    value, bit = 0, 1
    while bit < size:
        value = value + ((place // bit + mask // bit) % 2) * bit
        bit *= 2
    return value


def kernel(spaces, times, parts, x_ref, out_ref, held, arrived, tot, tots, ones,
           load_sem, main_send, main_recv, head_send, head_recv, tot_send, tot_recv, up, across, go):
    lat, days, lon = x_ref.shape
    block = lon // spaces
    rows = spaces // ROW
    low, high = rows // 2 - 1, rows // 2
    me = lax.axis_index("space")
    when = lax.axis_index("tm")
    z, y = me // ROW, me % ROW
    inner = (z == low) | (z == high)

    def pick(tables):
        return [a if a == b else jnp.where(inner, a, b) for a, b in zip(*tables)]

    sends = pick((INNER[spaces][0], OUTER[spaces][0]))
    turns = pick((INNER[spaces][1], OUTER[spaces][1]))

    def columns(place):
        return pl.ds(pl.multiple_of(place * block, block), block)

    order = [flip(me, step, spaces) for step in sends] + [me]
    pieces = len(parts)

    def load_of(place, at, size, k):
        span = pl.ds(at, size)
        return pltpu.make_async_copy(
            x_ref.at[span, :, columns(place)], held.at[span, :, columns(place)], load_sem.at[k]
        )

    loads = [load_of(order[0], at, size, k) for k, (at, size) in enumerate(parts)]
    loads += [load_of(place, 0, lat, pieces + k) for k, place in enumerate(order[1:])]

    barrier = pltpu.get_barrier_semaphore()

    def signal(semaphore, **place):
        pl.semaphore_signal(semaphore, inc=1, device_id=place, device_id_type=MESH)

    def ends(semaphore):
        for k in range(ROW):
            for j in range(times):
                if k or j:
                    signal(semaphore, space=(y + k) % ROW, tm=(when + j) % times)

    @pl.when(z < rows - 1)
    def _():
        signal(barrier, space=me + ROW)

    @pl.when((z > 0) & (z <= high))
    def _():
        signal(barrier, space=me - ROW)

    @pl.when(z == 0)
    def _():
        ends(barrier)

    for load in loads:
        load.start()
    group = ROW * times - 1
    pl.semaphore_wait(
        barrier, jnp.where(z > 0, 1, 0) + jnp.where(z <= low, 1, 0) + jnp.where(z == 0, group, 0)
    )

    def main(step, c):
        peer = flip(me, step, spaces)
        span = pl.ds(parts[c][0], parts[c][1])
        return pltpu.make_async_remote_copy(
            src_ref=held.at[span, pl.ds(HEAD, days - HEAD), columns(peer)],
            dst_ref=arrived.at[step - 1, span, pl.ds(HEAD, days - HEAD)],
            send_sem=main_send.at[step - 1, c],
            recv_sem=main_recv.at[step - 1, c],
            device_id={"space": peer},
            device_id_type=MESH,
        )

    def head(step):
        peer = flip(me, step, spaces)
        return pltpu.make_async_remote_copy(
            src_ref=held.at[:, pl.ds(0, HEAD), columns(peer)],
            dst_ref=arrived.at[step - 1, :, pl.ds(0, HEAD)],
            send_sem=head_send.at[step - 1],
            recv_sem=head_recv.at[step - 1],
            device_id={"space": peer},
            device_id_type=MESH,
        )

    def total(step):
        return pltpu.make_async_remote_copy(
            src_ref=tot,
            dst_ref=tots.at[step - 1],
            send_sem=tot_send.at[step - 1],
            recv_sem=tot_recv.at[step - 1],
            device_id={"tm": lax.rem(when + step, times)},
            device_id_type=MESH,
        )

    loads[0].wait()
    main(sends[0], 0).start()

    @pl.when(z < rows - 1)
    def _():
        pl.semaphore_wait(up, 1)

    @pl.when(z > 0)
    def _():
        signal(up, space=me - ROW)

    @pl.when(z == 0)
    def _():
        ends(across)
        pl.semaphore_wait(across, group)
        for k in range(1, rows):
            signal(go, space=me + k * ROW)

    for load in loads[1:]:
        load.wait()
    for a in range(lat):
        tot[a] = jnp.sum(held[a], axis=0, keepdims=True)
    position = lax.broadcasted_iota(jnp.int32, (days, days), 0)
    later = lax.broadcasted_iota(jnp.int32, (days, days), 1)
    ones[...] = (position <= later).astype(jnp.float32)

    @pl.when(z > 0)
    def _():
        pl.semaphore_wait(go, 1)

    for step in range(1, times):
        total(step).start()
    for step in sends[1:FIRST]:
        for c in range(pieces):
            main(step, c).start()
    for step in range(1, times):
        total(step).wait_recv()
    for a in range(lat):
        carry = jnp.zeros((1, lon), jnp.float32)
        for step in range(1, times):
            earlier = jnp.where(when >= step, 1.0, 0.0)
            carry = carry + tots[step - 1, a] * earlier
        held[a, 0:1, :] = held[a, 0:1, :] + carry

    def prefix(x):
        return lax.dot_general(
            x.T, ones[...], (((1,), (0,)), ((), ())),
            precision=lax.Precision.HIGHEST, preferred_element_type=jnp.float32,
        )

    for step in sends:
        head(step).start()
    for step in sends[FIRST:]:
        for c in range(pieces):
            main(step, c).start()
    for c in range(1, pieces):
        main(sends[0], c).start()

    @pl.loop(0, lat)
    def _(a):
        out_ref[me * lat + a] = prefix(held[a, :, columns(me)])

    def receive(step, c):
        source = flip(me, step, spaces)
        main(step, c).wait_recv()

        @pl.loop(parts[c][0], parts[c][0] + parts[c][1])
        def _(a):
            out_ref[source * lat + a] = prefix(arrived[step - 1, a])

    head(turns[0]).wait_recv()
    receive(turns[0], 0)
    for step in turns[1:]:
        head(step).wait_recv()
        for c in range(pieces):
            receive(step, c)

    for step in range(1, times):
        total(step).wait_send()
    for step in sends:
        head(step).wait_send()
        for c in range(pieces if step is not sends[0] else 1):
            main(step, c).wait_send()
    for c in range(1, pieces):
        receive(turns[0], c)
    for c in range(1, pieces):
        main(sends[0], c).wait_send()


def direct(spaces, times, precip):
    days, lat, lon = precip.shape
    parts = parts_of(lat)
    pieces = len(parts)
    block = lon // spaces
    rows = jnp.transpose(precip, (1, 0, 2))
    dma, plain_sem = pltpu.SemaphoreType.DMA, pltpu.SemaphoreType.REGULAR
    return pl.pallas_call(
        functools.partial(kernel, spaces, times, parts),
        out_shape=jax.ShapeDtypeStruct((lat * spaces, block, days), jnp.float32),
        in_specs=[pl.BlockSpec(memory_space=pltpu.HBM)],
        out_specs=pl.BlockSpec(memory_space=pltpu.VMEM),
        scratch_shapes=[
            pltpu.VMEM((lat, days, lon), jnp.float32),
            pltpu.VMEM((spaces - 1, lat, days, block), jnp.float32),
            pltpu.VMEM((lat, 1, lon), jnp.float32),
            pltpu.VMEM((times - 1, lat, 1, lon), jnp.float32),
            pltpu.VMEM((days, days), jnp.float32),
            dma((pieces + spaces - 1,)),
            dma((spaces - 1, pieces)),
            dma((spaces - 1, pieces)),
            dma((spaces - 1,)),
            dma((spaces - 1,)),
            dma((times - 1,)),
            dma((times - 1,)),
            plain_sem,
            plain_sem,
            plain_sem,
        ],
        compiler_params=pltpu.CompilerParams(
            collective_id=0, has_side_effects=True, vmem_limit_bytes=46 * 2**20
        ),
        name="rechunk",
    )(rows)


def plain(precip):
    days = precip.shape[0]
    position = lax.broadcasted_iota(jnp.int32, (days, days), 0)
    later = lax.broadcasted_iota(jnp.int32, (days, days), 1)
    ones = (position <= later).astype(jnp.float32)
    source = lax.all_to_all(precip, "space", split_axis=2, concat_axis=1, tiled=True)
    pixel_major = jnp.transpose(source, (1, 2, 0))
    running = jnp.dot(
        pixel_major, ones, precision=lax.Precision.HIGHEST, preferred_element_type=jnp.float32
    )
    last = lax.all_gather(running[:, :, -1], "tm")
    place = lax.broadcasted_iota(jnp.int32, last.shape, 0)
    carried = jnp.sum(jnp.where(place < lax.axis_index("tm"), last, 0.0), axis=0)
    return running + carried[:, :, None]


def solution(mesh):
    spaces, times = mesh.shape["space"], mesh.shape["tm"]

    def per_device(precip):
        days, _, lon = precip.shape
        tiled = lon % (spaces * 128) == 0 and days % 128 == 0
        if tiled and spaces in INNER and times > 1:
            return direct(spaces, times, precip)
        return plain(precip)

    return jax.shard_map(
        per_device,
        mesh=mesh,
        in_specs=(P("tm", "space", None),),
        out_specs=P(None, "space", "tm"),
        check_vma=False,
    )
```

```python
import functools

import jax
import jax.numpy as jnp
from jax import lax
from jax.experimental import pallas as pl
from jax.experimental.pallas import tpu as pltpu
from jax.sharding import PartitionSpec as P

MESH = pl.DeviceIdType.MESH
HEAD = 8
ROW = 2
SPLIT, LAST = 6, 7
STEPS = {
    (True, 0): ((), (5, 4, 2, 3), (), (1,), (2, 3, 1, 5, 4)),
    (True, 1): ((), (2, 3), (), (5, 4, 1), (2, 3, 1, 5, 4)),
    (False, 0): ((2,), (3,), (1, 5, 4, 7, 6), (), (2, 3, 5, 4, 1, 7, 6)),
    (False, 1): ((2,), (3,), (1, 7, 6, 5, 4), (), (2, 3, 1, 5, 4, 7, 6)),
}
SPACES = 8
PARTS = (3, 2, 1)
GRANT = 44 * 2**20


def parts_of(lat):
    total = sum(PARTS)
    if lat % total:
        return ((0, lat),)
    unit, at, found = lat // total, 0, []
    for part in PARTS:
        found.append((at, part * unit))
        at += part * unit
    return tuple(found)


def flip(place, mask, size):
    value, bit = 0, 1
    while bit < size:
        value = value + ((place // bit + mask // bit) % 2) * bit
        bit *= 2
    return value


def prefix(x, ones):
    return lax.dot_general(
        x.T, ones[...], (((1,), (0,)), ((), ())),
        precision=lax.Precision.HIGHEST, preferred_element_type=jnp.float32,
    )


def upper(ones):
    position = lax.broadcasted_iota(jnp.int32, ones.shape, 0)
    later = lax.broadcasted_iota(jnp.int32, ones.shape, 1)
    ones[...] = (position <= later).astype(jnp.float32)


def by_kind(inner, when, act):
    for (within, core) in STEPS:
        side = inner if within else jnp.logical_not(inner)
        pl.when(side & (when % 2 == core))(functools.partial(act, within, core))


def most(spaces, times, early, x_ref, out_ref, kept, held, arrived, tot, tots, ones,
         load_sem, sent, main_recv, piece_sent, piece_recv, head_recv, tot_send, tot_recv, up, across, go):
    lat, days, lon = x_ref.shape
    block = lon // spaces
    rows = spaces // ROW
    low, high = rows // 2 - 1, rows // 2
    me = lax.axis_index("space")
    when = lax.axis_index("tm")
    z, y = me // ROW, me % ROW
    inner = (z == low) | (z == high)

    def columns(place):
        return pl.ds(pl.multiple_of(place * block, block), block)

    order = [SPLIT, *(k for k in range(1, spaces) if k != SPLIT)]
    order = [flip(me, step, spaces) for step in order] + [me]

    def load_of(place, at, size, k):
        span = pl.ds(at, size)
        return pltpu.make_async_copy(
            x_ref.at[span, :, columns(place)], held.at[span, :, columns(place)], load_sem.at[k]
        )

    loads = [load_of(order[0], 0, early, 0), load_of(order[0], early, lat - early, 1)]
    loads += [load_of(place, 0, lat, 2) for place in order[1:]]

    barrier = pltpu.get_barrier_semaphore()

    def signal(semaphore, **place):
        pl.semaphore_signal(semaphore, inc=1, device_id=place, device_id_type=MESH)

    def ends(semaphore):
        for k in range(ROW):
            for j in range(times):
                if k or j:
                    signal(semaphore, space=(y + k) % ROW, tm=(when + j) % times)

    @pl.when(z < rows - 1)
    def _():
        signal(barrier, space=me + ROW)

    @pl.when((z > 0) & (z <= high))
    def _():
        signal(barrier, space=me - ROW)

    @pl.when(z == 0)
    def _():
        ends(barrier)

    for load in loads:
        load.start()
    group = ROW * times - 1
    pl.semaphore_wait(
        barrier, jnp.where(z > 0, 1, 0) + jnp.where(z <= low, 1, 0) + jnp.where(z == 0, group, 0)
    )

    def block_copy(step, at_day, size, rows_in, send_sem, recv_sem):
        peer = flip(me, step, spaces)
        span, time = pl.ds(0, rows_in), pl.ds(at_day, size)
        return pltpu.make_async_remote_copy(
            src_ref=held.at[span, time, columns(peer)],
            dst_ref=arrived.at[step - 1, span, time],
            send_sem=send_sem,
            recv_sem=recv_sem,
            device_id={"space": peer},
            device_id_type=MESH,
        )

    def main(step):
        return block_copy(step, HEAD, days - HEAD, lat, sent, main_recv.at[step - 1])

    def head(step):
        return block_copy(step, 0, HEAD, lat, sent, head_recv.at[step - 1])

    def piece():
        return block_copy(SPLIT, HEAD, days - HEAD, early, piece_sent, piece_recv.at[0])

    def piece_head():
        return block_copy(SPLIT, 0, HEAD, early, piece_sent, piece_recv.at[1])

    def total(step):
        return pltpu.make_async_remote_copy(
            src_ref=tot,
            dst_ref=tots.at[step - 1],
            send_sem=tot_send,
            recv_sem=tot_recv.at[step - 1],
            device_id={"tm": lax.rem(when + step, times)},
            device_id_type=MESH,
        )

    def send(k):
        def act(within, core):
            for step in STEPS[within, core][k]:
                main(step).start()

        by_kind(inner, when, act)

    loads[0].wait()

    @pl.when(inner)
    def _():
        piece().start()

    @pl.when(z < rows - 1)
    def _():
        pl.semaphore_wait(up, 1)

    @pl.when(z > 0)
    def _():
        signal(up, space=me - ROW)

    @pl.when(z == 0)
    def _():
        ends(across)
        pl.semaphore_wait(across, group)
        for k in range(1, rows):
            signal(go, space=me + k * ROW)

    loads[1].wait()
    pltpu.make_async_copy(arrived, arrived, load_sem.at[2]).wait()
    send(0)
    for a in range(lat):
        tot[a] = jnp.sum(held[a], axis=0, keepdims=True)
    upper(ones)

    @pl.when(z > 0)
    def _():
        pl.semaphore_wait(go, 1)

    for step in range(1, times):
        total(step).start()
    send(1)
    for step in range(1, times):
        total(step).wait_recv()
    for a in range(lat):
        carry = jnp.zeros((1, lon), jnp.float32)
        for step in range(1, times):
            earlier = jnp.where(when >= step, 1.0, 0.0)
            carry = carry + tots[step - 1, a] * earlier
        held[a, 0:1, :] = held[a, 0:1, :] + carry

    def heads(within, core):
        if within:
            piece_head().start()
        for batch in STEPS[within, core][:4]:
            for step in batch:
                head(step).start()

    by_kind(inner, when, heads)
    send(2)
    for k, step in enumerate((LAST, SPLIT)):
        place = columns(flip(me, step, spaces))

        @pl.loop(0, lat)
        def _(a):
            kept[k, a] = held[a, :, place]

    def put(source, k, rows_in):
        @pl.loop(0, rows_in)
        def _(a):
            out_ref[source * lat + a] = prefix(arrived[k, a], ones)

    @pl.loop(0, lat)
    def _(a):
        out_ref[me * lat + a] = prefix(held[a, :, columns(me)], ones)

    def arrivals(within, core):
        steps = STEPS[within, core][4]
        if within:
            main(steps[0]).wait_recv()
            for step in STEPS[within, core][3]:
                main(step).start()
            piece_head().wait_recv()
            piece().wait_recv()
            put(flip(me, SPLIT, spaces), SPLIT - 1, early)
        for step in steps:
            head(step).wait_recv()
            if not within or step != steps[0]:
                main(step).wait_recv()
            put(flip(me, step, spaces), step - 1, lat)
        count = sum(len(batch) for batch in STEPS[within, core][:4])
        blocks = arrived.at[pl.ds(0, count)]
        pltpu.make_async_copy(blocks, blocks, sent).wait()
        if within:
            rows_out = arrived.at[0, pl.ds(0, early)]
            pltpu.make_async_copy(rows_out, rows_out, piece_sent).wait()

    by_kind(inner, when, arrivals)
    pltpu.make_async_copy(tots, tots, tot_send).wait()


def put_away(first_ref, out_ref, token_ref, sem):
    copy = pltpu.make_async_copy(first_ref, out_ref, sem)
    copy.start()
    token_ref[...] = jnp.zeros_like(token_ref)
    copy.wait()


def rest(spaces, lat, parts, token_ref, kept, out_ref, got, ones, sent, received):
    days, block = got.shape[1:]
    me = lax.axis_index("space")
    z = me // ROW
    inner = (z == spaces // ROW // 2 - 1) | (z == spaces // ROW // 2)
    barrier = pltpu.get_barrier_semaphore()

    @pl.when(inner)
    def _():
        for step in (LAST, SPLIT):
            pl.semaphore_signal(
                barrier, inc=1, device_id={"space": flip(me, step, spaces)}, device_id_type=MESH
            )
        upper(ones)
        pl.semaphore_wait(barrier, 2)

    def copy(step, at, size, to, send_sem, recv_sem):
        peer = flip(me, step, spaces)
        return pltpu.make_async_remote_copy(
            src_ref=kept.at[(LAST, SPLIT).index(step), pl.ds(at, size)],
            dst_ref=got.at[pl.ds(to, size)],
            send_sem=send_sem,
            recv_sem=recv_sem,
            device_id={"space": peer},
            device_id_type=MESH,
        )

    whole = copy(LAST, 0, lat, 0, sent.at[0], received.at[0])
    at, pieces = lat, []
    for k, (start, size) in enumerate(parts[1:]):
        pieces.append((at, size, copy(SPLIT, start, size, at, sent.at[1 + k], received.at[1 + k])))
        at += size

    def put(at, size):
        @pl.loop(at, at + size)
        def _(a):
            out_ref[a] = prefix(got[a], ones)

    @pl.when(inner)
    def _():
        whole.start()
        for _, _, piece in pieces:
            piece.start()
        whole.wait_recv()
        put(0, lat)
        for k, (at, size, piece) in enumerate(pieces):
            piece.wait_recv()
            put(at, size)
        whole.wait_send()
        for _, _, piece in pieces:
            piece.wait_send()


def finish(spaces, lat, parts, all_ref, late_ref, out_ref, sem):
    me = lax.axis_index("space")
    z = me // ROW
    inner = (z == spaces // ROW // 2 - 1) | (z == spaces // ROW // 2)
    start = parts[1][0]

    def copy(step, at, to, size, k):
        return pltpu.make_async_copy(
            late_ref.at[pl.ds(at, size)],
            out_ref.at[pl.ds(flip(me, step, spaces) * lat + to, size)],
            sem.at[k],
        )

    @pl.when(inner)
    def _():
        copies = [copy(LAST, 0, 0, lat, 0), copy(SPLIT, lat, start, lat - start, 1)]
        for c in copies:
            c.start()
        for c in copies:
            c.wait()


def direct(spaces, times, precip):
    days, lat, lon = precip.shape
    parts = parts_of(lat)
    early = parts[0][1]
    late = lat + sum(size for _, size in parts[1:])
    block = lon // spaces
    rows = jnp.transpose(precip, (1, 0, 2))
    dma, plain_sem = pltpu.SemaphoreType.DMA, pltpu.SemaphoreType.REGULAR
    vmem, hbm = pl.BlockSpec(memory_space=pltpu.VMEM), pl.BlockSpec(memory_space=pltpu.HBM)

    def shaped(*shape):
        return jax.ShapeDtypeStruct(shape, jnp.float32)

    first, blocks = pl.pallas_call(
        functools.partial(most, spaces, times, early),
        out_shape=(shaped(lat * spaces, block, days), shaped(2, lat, days, block)),
        in_specs=[hbm],
        out_specs=(vmem, vmem),
        scratch_shapes=[
            pltpu.VMEM((lat, days, lon), jnp.float32),
            pltpu.VMEM((spaces - 1, lat, days, block), jnp.float32),
            pltpu.VMEM((lat, 1, lon), jnp.float32),
            pltpu.VMEM((times - 1, lat, 1, lon), jnp.float32),
            pltpu.VMEM((days, days), jnp.float32),
            dma((3,)),
            dma,
            dma((spaces - 1,)),
            dma,
            dma((2,)),
            dma((spaces - 1,)),
            dma,
            dma((times - 1,)),
            plain_sem,
            plain_sem,
            plain_sem,
        ],
        compiler_params=pltpu.CompilerParams(
            collective_id=0, has_side_effects=True, vmem_limit_bytes=GRANT
        ),
        name="most",
    )(rows)
    whole, token = pl.pallas_call(
        put_away,
        out_shape=(shaped(lat * spaces, block, days), shaped(8, 128)),
        in_specs=[vmem],
        out_specs=(hbm, vmem),
        scratch_shapes=[dma],
        compiler_params=pltpu.CompilerParams(vmem_limit_bytes=GRANT),
        name="put_away",
    )(first)
    more = pl.pallas_call(
        functools.partial(rest, spaces, lat, parts),
        out_shape=shaped(late, block, days),
        in_specs=[vmem, vmem],
        out_specs=vmem,
        scratch_shapes=[
            pltpu.VMEM((late, days, block), jnp.float32),
            pltpu.VMEM((days, days), jnp.float32),
            dma((len(parts),)),
            dma((len(parts),)),
        ],
        compiler_params=pltpu.CompilerParams(
            collective_id=1, has_side_effects=True, vmem_limit_bytes=GRANT
        ),
        name="rest",
    )(token, blocks)
    return pl.pallas_call(
        functools.partial(finish, spaces, lat, parts),
        out_shape=shaped(lat * spaces, block, days),
        in_specs=[hbm, vmem],
        out_specs=hbm,
        input_output_aliases={0: 0},
        scratch_shapes=[dma((2,))],
        compiler_params=pltpu.CompilerParams(vmem_limit_bytes=GRANT),
        name="finish",
    )(whole, more)


def plain(precip):
    days = precip.shape[0]
    position = lax.broadcasted_iota(jnp.int32, (days, days), 0)
    later = lax.broadcasted_iota(jnp.int32, (days, days), 1)
    ones = (position <= later).astype(jnp.float32)
    source = lax.all_to_all(precip, "space", split_axis=2, concat_axis=1, tiled=True)
    pixel_major = jnp.transpose(source, (1, 2, 0))
    running = jnp.dot(
        pixel_major, ones, precision=lax.Precision.HIGHEST, preferred_element_type=jnp.float32
    )
    last = lax.all_gather(running[:, :, -1], "tm")
    place = lax.broadcasted_iota(jnp.int32, last.shape, 0)
    carried = jnp.sum(jnp.where(place < lax.axis_index("tm"), last, 0.0), axis=0)
    return running + carried[:, :, None]


def solution(mesh):
    spaces, times = mesh.shape["space"], mesh.shape["tm"]

    def per_device(precip):
        days, lat, lon = precip.shape
        tiled = lon % (spaces * 128) == 0 and days % 128 == 0
        if tiled and lat % sum(PARTS) == 0 and spaces == SPACES and times > 1 and times % 2 == 0:
            return direct(spaces, times, precip)
        return plain(precip)

    return jax.shard_map(
        per_device,
        mesh=mesh,
        in_specs=(P("tm", "space", None),),
        out_specs=P(None, "space", "tm"),
        check_vma=False,
    )
```

```python
import functools

import jax
import jax.numpy as jnp
from jax import lax
from jax.experimental import pallas as pl
from jax.experimental.pallas import tpu as pltpu
from jax.sharding import PartitionSpec as P

MESH = pl.DeviceIdType.MESH
HEAD = 8
ROW = 2
SPLIT, LAST = 6, 7
STEPS = {
    (True, 0): ((2,), (4, 5, 3), (), (1,), (), (2, 3, 1, 5, 4)),
    (True, 1): ((), (), (), (5, 4, 2, 1), (3,), (2, 3, 1, 5, 4)),
    (False, 0): ((2,), (3,), (1, 5, 4, 6, 7), (), (), (2, 3, 5, 4, 1, 6, 7)),
    (False, 1): ((2,), (3,), (1, 6, 7, 4, 5), (), (), (2, 3, 1, 5, 4, 6, 7)),
}
SPACES = 8
PARTS = (3, 2, 1)
GRANT = 44 * 2**20


def parts_of(lat):
    total = sum(PARTS)
    if lat % total:
        return ((0, lat),)
    unit, at, found = lat // total, 0, []
    for part in PARTS:
        found.append((at, part * unit))
        at += part * unit
    return tuple(found)


def flip(place, mask, size):
    value, bit = 0, 1
    while bit < size:
        value = value + ((place // bit + mask // bit) % 2) * bit
        bit *= 2
    return value


def prefix(x, ones):
    return lax.dot_general(
        x.T, ones[...], (((1,), (0,)), ((), ())),
        precision=lax.Precision.HIGHEST, preferred_element_type=jnp.float32,
    )


def upper(ones):
    position = lax.broadcasted_iota(jnp.int32, ones.shape, 0)
    later = lax.broadcasted_iota(jnp.int32, ones.shape, 1)
    ones[...] = (position <= later).astype(jnp.float32)


def by_kind(inner, when, act):
    for (within, core) in STEPS:
        side = inner if within else jnp.logical_not(inner)
        pl.when(side & (when % 2 == core))(functools.partial(act, within, core))


def most(spaces, times, unit, early, x_ref, out_ref, kept, held, arrived, tot, tots, ones,
         load_sem, sent, main_recv, piece_sent, piece_recv, head_recv, tot_send, tot_recv, up, across, go):
    lat, days, lon = x_ref.shape
    block = lon // spaces
    rows = spaces // ROW
    low, high = rows // 2 - 1, rows // 2
    me = lax.axis_index("space")
    when = lax.axis_index("tm")
    z, y = me // ROW, me % ROW
    inner = (z == low) | (z == high)

    def columns(place):
        return pl.ds(pl.multiple_of(place * block, block), block)

    order = [SPLIT, *(k for k in range(1, spaces) if k != SPLIT)]
    order = [flip(me, step, spaces) for step in order] + [me]

    def load_of(place, at, size, k):
        span = pl.ds(at, size)
        return pltpu.make_async_copy(
            x_ref.at[span, :, columns(place)], held.at[span, :, columns(place)], load_sem.at[k]
        )

    cuts = (0, unit, early, lat)
    loads = [load_of(order[0], at, to - at, k) for k, (at, to) in enumerate(zip(cuts, cuts[1:]))]
    loads += [load_of(place, 0, lat, len(loads)) for place in order[1:]]

    barrier = pltpu.get_barrier_semaphore()

    def signal(semaphore, **place):
        pl.semaphore_signal(semaphore, inc=1, device_id=place, device_id_type=MESH)

    def ends(semaphore):
        for k in range(ROW):
            for j in range(times):
                if k or j:
                    signal(semaphore, space=(y + k) % ROW, tm=(when + j) % times)

    @pl.when(z < rows - 1)
    def _():
        signal(barrier, space=me + ROW)

    @pl.when((z > 0) & (z <= high))
    def _():
        signal(barrier, space=me - ROW)

    @pl.when(z == 0)
    def _():
        ends(barrier)

    for load in loads:
        load.start()
    group = ROW * times - 1
    pl.semaphore_wait(
        barrier, jnp.where(z > 0, 1, 0) + jnp.where(z <= low, 1, 0) + jnp.where(z == 0, group, 0)
    )

    def block_copy(step, at_day, size, rows_in, send_sem, recv_sem, at=0):
        peer = flip(me, step, spaces)
        span, time = pl.ds(at, rows_in), pl.ds(at_day, size)
        return pltpu.make_async_remote_copy(
            src_ref=held.at[span, time, columns(peer)],
            dst_ref=arrived.at[step - 1, span, time],
            send_sem=send_sem,
            recv_sem=recv_sem,
            device_id={"space": peer},
            device_id_type=MESH,
        )

    def main(step):
        return block_copy(step, HEAD, days - HEAD, lat, sent, main_recv.at[step - 1])

    def head(step):
        return block_copy(step, 0, HEAD, lat, sent, head_recv.at[step - 1])

    def piece(k):
        size = cuts[k + 1] - cuts[k]
        return block_copy(SPLIT, HEAD, days - HEAD, size, piece_sent, piece_recv.at[k], cuts[k])

    def piece_head():
        return block_copy(SPLIT, 0, HEAD, early, piece_sent, piece_recv.at[2])

    def total(step):
        return pltpu.make_async_remote_copy(
            src_ref=tot,
            dst_ref=tots.at[step - 1],
            send_sem=tot_send,
            recv_sem=tot_recv.at[step - 1],
            device_id={"tm": lax.rem(when + step, times)},
            device_id_type=MESH,
        )

    def send(k):
        def act(within, core):
            for step in STEPS[within, core][k]:
                main(step).start()

        by_kind(inner, when, act)

    for k in range(2):
        loads[k].wait()

        @pl.when(inner)
        def _():
            piece(k).start()

    @pl.when(z < rows - 1)
    def _():
        pl.semaphore_wait(up, 1)

    @pl.when(z > 0)
    def _():
        signal(up, space=me - ROW)

    @pl.when(z == 0)
    def _():
        ends(across)
        pl.semaphore_wait(across, group)
        for k in range(1, rows):
            signal(go, space=me + k * ROW)

    loads[2].wait()
    pltpu.make_async_copy(arrived, arrived, load_sem.at[3]).wait()
    send(0)
    for a in range(lat):
        tot[a] = jnp.sum(held[a], axis=0, keepdims=True)
    upper(ones)

    @pl.when(z > 0)
    def _():
        pl.semaphore_wait(go, 1)

    for step in range(1, times):
        total(step).start()
    send(1)
    for step in range(1, times):
        total(step).wait_recv()
    for a in range(lat):
        carry = jnp.zeros((1, lon), jnp.float32)
        for step in range(1, times):
            earlier = jnp.where(when >= step, 1.0, 0.0)
            carry = carry + tots[step - 1, a] * earlier
        held[a, 0:1, :] = held[a, 0:1, :] + carry

    def heads(within, core):
        if within:
            piece_head().start()
        for batch in STEPS[within, core][:5]:
            for step in batch:
                head(step).start()

    by_kind(inner, when, heads)
    send(2)
    for k, step in enumerate((LAST, SPLIT)):
        place = columns(flip(me, step, spaces))

        @pl.loop(0, lat)
        def _(a):
            kept[k, a] = held[a, :, place]

    def put(source, k, rows_in):
        @pl.loop(0, rows_in)
        def _(a):
            out_ref[source * lat + a] = prefix(arrived[k, a], ones)

    @pl.loop(0, lat)
    def _(a):
        out_ref[me * lat + a] = prefix(held[a, :, columns(me)], ones)

    def arrivals(within, core):
        steps = STEPS[within, core][5]
        if within:
            main(steps[0]).wait_recv()
            for step in STEPS[within, core][3]:
                main(step).start()
            piece_head().wait_recv()
            for k in range(2):
                piece(k).wait_recv()
            put(flip(me, SPLIT, spaces), SPLIT - 1, early)
        for step in steps:
            head(step).wait_recv()
            if not within or step != steps[0]:
                main(step).wait_recv()
            put(flip(me, step, spaces), step - 1, lat)
            if step == steps[0]:
                for other in STEPS[within, core][4]:
                    main(other).start()
        count = sum(len(batch) for batch in STEPS[within, core][:5])
        blocks = arrived.at[pl.ds(0, count)]
        pltpu.make_async_copy(blocks, blocks, sent).wait()
        if within:
            rows_out = arrived.at[0, pl.ds(0, early)]
            pltpu.make_async_copy(rows_out, rows_out, piece_sent).wait()

    by_kind(inner, when, arrivals)
    pltpu.make_async_copy(tots, tots, tot_send).wait()


def put_away(first_ref, out_ref, token_ref, sem):
    copy = pltpu.make_async_copy(first_ref, out_ref, sem)
    copy.start()
    token_ref[...] = jnp.zeros_like(token_ref)
    copy.wait()


def rest(spaces, lat, parts, token_ref, kept, out_ref, raw, got, ones, sent, received):
    days, block = got.shape[1:]
    me = lax.axis_index("space")
    z = me // ROW
    inner = (z == spaces // ROW // 2 - 1) | (z == spaces // ROW // 2)
    barrier = pltpu.get_barrier_semaphore()

    @pl.when(inner)
    def _():
        for step in (LAST, SPLIT):
            pl.semaphore_signal(
                barrier, inc=1, device_id={"space": flip(me, step, spaces)}, device_id_type=MESH
            )
        upper(ones)
        pl.semaphore_wait(barrier, 2)

    def copy(step, at, size, to, send_sem, recv_sem, into=got):
        peer = flip(me, step, spaces)
        return pltpu.make_async_remote_copy(
            src_ref=kept.at[(LAST, SPLIT).index(step), pl.ds(at, size)],
            dst_ref=into.at[pl.ds(to, size)],
            send_sem=send_sem,
            recv_sem=recv_sem,
            device_id={"space": peer},
            device_id_type=MESH,
        )

    whole = copy(LAST, 0, lat, 0, sent.at[0], received.at[0])
    at, pieces = lat, []
    for k, (start, size) in enumerate(parts[1:-1]):
        pieces.append((at, size, copy(SPLIT, start, size, at, sent.at[1 + k], received.at[1 + k])))
        at += size
    k = len(parts) - 1
    final = copy(SPLIT, *parts[-1], 0, sent.at[k], received.at[k], raw)

    def put(at, size):
        @pl.loop(at, at + size)
        def _(a):
            out_ref[a] = prefix(got[a], ones)

    @pl.when(inner)
    def _():
        whole.start()
        for _, _, piece in pieces:
            piece.start()
        final.start()
        whole.wait_recv()
        put(0, lat)
        for k, (at, size, piece) in enumerate(pieces):
            piece.wait_recv()
            put(at, size)
        whole.wait_send()
        for _, _, piece in pieces:
            piece.wait_send()
        final.wait()


def finish(spaces, lat, parts, all_ref, late_ref, raw_ref, out_ref, done, ones, sem):
    me = lax.axis_index("space")
    z = me // ROW
    inner = (z == spaces // ROW // 2 - 1) | (z == spaces // ROW // 2)
    start, end, last = parts[1][0], *parts[-1]

    def copy(from_ref, step, at, to, size, k):
        place = flip(me, step, spaces) * lat + to
        return pltpu.make_async_copy(
            from_ref.at[pl.ds(at, size)], out_ref.at[pl.ds(place, size)], sem.at[k]
        )

    @pl.when(inner)
    def _():
        copies = [copy(late_ref, LAST, 0, 0, lat, 0), copy(late_ref, SPLIT, lat, start, end - start, 1)]
        for c in copies:
            c.start()
        upper(ones)
        for a in range(last):
            done[a] = prefix(raw_ref[a], ones)
        copies.append(copy(done, SPLIT, 0, end, last, 2))
        copies[-1].start()
        for c in copies:
            c.wait()


def direct(spaces, times, precip):
    days, lat, lon = precip.shape
    parts = parts_of(lat)
    early = parts[0][1]
    late = lat + sum(size for _, size in parts[1:-1])
    last = parts[-1][1]
    block = lon // spaces
    rows = jnp.transpose(precip, (1, 0, 2))
    dma, plain_sem = pltpu.SemaphoreType.DMA, pltpu.SemaphoreType.REGULAR
    vmem, hbm = pl.BlockSpec(memory_space=pltpu.VMEM), pl.BlockSpec(memory_space=pltpu.HBM)

    def shaped(*shape):
        return jax.ShapeDtypeStruct(shape, jnp.float32)

    first, blocks = pl.pallas_call(
        functools.partial(most, spaces, times, lat // sum(PARTS), early),
        out_shape=(shaped(lat * spaces, block, days), shaped(2, lat, days, block)),
        in_specs=[hbm],
        out_specs=(vmem, vmem),
        scratch_shapes=[
            pltpu.VMEM((lat, days, lon), jnp.float32),
            pltpu.VMEM((spaces - 1, lat, days, block), jnp.float32),
            pltpu.VMEM((lat, 1, lon), jnp.float32),
            pltpu.VMEM((times - 1, lat, 1, lon), jnp.float32),
            pltpu.VMEM((days, days), jnp.float32),
            dma((4,)),
            dma,
            dma((spaces - 1,)),
            dma,
            dma((3,)),
            dma((spaces - 1,)),
            dma,
            dma((times - 1,)),
            plain_sem,
            plain_sem,
            plain_sem,
        ],
        compiler_params=pltpu.CompilerParams(
            collective_id=0, has_side_effects=True, vmem_limit_bytes=GRANT
        ),
        name="most",
    )(rows)
    whole, token = pl.pallas_call(
        put_away,
        out_shape=(shaped(lat * spaces, block, days), shaped(8, 128)),
        in_specs=[vmem],
        out_specs=(hbm, vmem),
        scratch_shapes=[dma],
        compiler_params=pltpu.CompilerParams(vmem_limit_bytes=GRANT),
        name="put_away",
    )(first)
    more, raw = pl.pallas_call(
        functools.partial(rest, spaces, lat, parts),
        out_shape=(shaped(late, block, days), shaped(last, days, block)),
        in_specs=[vmem, vmem],
        out_specs=(vmem, vmem),
        scratch_shapes=[
            pltpu.VMEM((late, days, block), jnp.float32),
            pltpu.VMEM((days, days), jnp.float32),
            dma((len(parts),)),
            dma((len(parts),)),
        ],
        compiler_params=pltpu.CompilerParams(
            collective_id=1, has_side_effects=True, vmem_limit_bytes=GRANT
        ),
        name="rest",
    )(token, blocks)
    return pl.pallas_call(
        functools.partial(finish, spaces, lat, parts),
        out_shape=shaped(lat * spaces, block, days),
        in_specs=[hbm, vmem, vmem],
        out_specs=hbm,
        input_output_aliases={0: 0},
        scratch_shapes=[
            pltpu.VMEM((last, block, days), jnp.float32),
            pltpu.VMEM((days, days), jnp.float32),
            dma((3,)),
        ],
        compiler_params=pltpu.CompilerParams(vmem_limit_bytes=GRANT),
        name="finish",
    )(whole, more, raw)


def plain(precip):
    days = precip.shape[0]
    position = lax.broadcasted_iota(jnp.int32, (days, days), 0)
    later = lax.broadcasted_iota(jnp.int32, (days, days), 1)
    ones = (position <= later).astype(jnp.float32)
    source = lax.all_to_all(precip, "space", split_axis=2, concat_axis=1, tiled=True)
    pixel_major = jnp.transpose(source, (1, 2, 0))
    running = jnp.dot(
        pixel_major, ones, precision=lax.Precision.HIGHEST, preferred_element_type=jnp.float32
    )
    last = lax.all_gather(running[:, :, -1], "tm")
    place = lax.broadcasted_iota(jnp.int32, last.shape, 0)
    carried = jnp.sum(jnp.where(place < lax.axis_index("tm"), last, 0.0), axis=0)
    return running + carried[:, :, None]


def solution(mesh):
    spaces, times = mesh.shape["space"], mesh.shape["tm"]

    def per_device(precip):
        days, lat, lon = precip.shape
        tiled = lon % (spaces * 128) == 0 and days % 128 == 0
        if tiled and lat % sum(PARTS) == 0 and spaces == SPACES and times > 1 and times % 2 == 0:
            return direct(spaces, times, precip)
        return plain(precip)

    return jax.shard_map(
        per_device,
        mesh=mesh,
        in_specs=(P("tm", "space", None),),
        out_specs=P(None, "space", "tm"),
        check_vma=False,
    )
```

```python
import functools

import jax
import jax.numpy as jnp
from jax import lax
from jax.experimental import pallas as pl
from jax.experimental.pallas import tpu as pltpu
from jax.sharding import PartitionSpec as P

MESH = pl.DeviceIdType.MESH
HEAD = 8
ROW = 2
SPLIT, LAST = 6, 7
STEPS = {
    (True, 0): ((4, 2), (5,), (), (3, 1), (), (2, 3, 1, 5, 4)),
    (True, 1): ((), (), (), (5, 4, 2, 1), (3,), (2, 3, 1, 5, 4)),
    (False, 0): ((2,), (3,), (5, 4, 6, 7), (), (1,), (2, 3, 5, 4, 6, 7, 1)),
    (False, 1): ((2,), (3,), (6, 7, 4, 5), (), (1,), (2, 3, 5, 4, 6, 7, 1)),
}
SPACES = 8
PARTS = (3, 2, 1)
GRANT = 44 * 2**20


def parts_of(lat):
    total = sum(PARTS)
    if lat % total:
        return ((0, lat),)
    unit, at, found = lat // total, 0, []
    for part in PARTS:
        found.append((at, part * unit))
        at += part * unit
    return tuple(found)


def flip(place, mask, size):
    value, bit = 0, 1
    while bit < size:
        value = value + ((place // bit + mask // bit) % 2) * bit
        bit *= 2
    return value


def prefix(x, ones):
    return lax.dot_general(
        x.T, ones[...], (((1,), (0,)), ((), ())),
        precision=lax.Precision.HIGHEST, preferred_element_type=jnp.float32,
    )


def upper(ones):
    position = lax.broadcasted_iota(jnp.int32, ones.shape, 0)
    later = lax.broadcasted_iota(jnp.int32, ones.shape, 1)
    ones[...] = (position <= later).astype(jnp.float32)


def by_kind(inner, when, act):
    for (within, core) in STEPS:
        side = inner if within else jnp.logical_not(inner)
        pl.when(side & (when % 2 == core))(functools.partial(act, within, core))


def most(spaces, times, unit, early, x_ref, out_ref, kept, held, arrived, tot, tots, ones,
         load_sem, sent, main_recv, piece_sent, piece_recv, head_recv, tot_send, tot_recv, up, down, across, go):
    lat, days, lon = x_ref.shape
    block = lon // spaces
    rows = spaces // ROW
    low, high = rows // 2 - 1, rows // 2
    me = lax.axis_index("space")
    when = lax.axis_index("tm")
    z, y = me // ROW, me % ROW
    inner = (z == low) | (z == high)

    def columns(place):
        return pl.ds(pl.multiple_of(place * block, block), block)

    order = [SPLIT, *(k for k in range(1, spaces) if k != SPLIT)]
    order = [flip(me, step, spaces) for step in order] + [me]

    def load_of(place, at, size, k):
        span = pl.ds(at, size)
        return pltpu.make_async_copy(
            x_ref.at[span, :, columns(place)], held.at[span, :, columns(place)], load_sem.at[k]
        )

    cuts = (0, unit, early, lat)
    loads = [load_of(order[0], at, to - at, k) for k, (at, to) in enumerate(zip(cuts, cuts[1:]))]
    loads += [load_of(place, 0, lat, len(loads)) for place in order[1:]]

    barrier = pltpu.get_barrier_semaphore()

    def signal(semaphore, **place):
        pl.semaphore_signal(semaphore, inc=1, device_id=place, device_id_type=MESH)

    def ends(semaphore):
        for k in range(ROW):
            for j in range(times):
                if k or j:
                    signal(semaphore, space=(y + k) % ROW, tm=(when + j) % times)

    @pl.when(z < rows - 1)
    def _():
        signal(barrier, space=me + ROW)

    @pl.when((z > 0) & (z <= high))
    def _():
        signal(barrier, space=me - ROW)

    @pl.when(z == 0)
    def _():
        ends(barrier)

    for load in loads:
        load.start()
    group = ROW * times - 1
    pl.semaphore_wait(
        barrier, jnp.where(z > 0, 1, 0) + jnp.where(z <= low, 1, 0) + jnp.where(z == 0, group, 0)
    )

    def block_copy(step, at_day, size, rows_in, send_sem, recv_sem, at=0):
        peer = flip(me, step, spaces)
        span, time = pl.ds(at, rows_in), pl.ds(at_day, size)
        return pltpu.make_async_remote_copy(
            src_ref=held.at[span, time, columns(peer)],
            dst_ref=arrived.at[step - 1, span, time],
            send_sem=send_sem,
            recv_sem=recv_sem,
            device_id={"space": peer},
            device_id_type=MESH,
        )

    def main(step):
        return block_copy(step, HEAD, days - HEAD, lat, sent, main_recv.at[step - 1])

    def head(step):
        return block_copy(step, 0, HEAD, lat, sent, head_recv.at[step - 1])

    def piece(k):
        size = cuts[k + 1] - cuts[k]
        return block_copy(SPLIT, HEAD, days - HEAD, size, piece_sent, piece_recv.at[k], cuts[k])

    def piece_head():
        return block_copy(SPLIT, 0, HEAD, early, piece_sent, piece_recv.at[2])

    def total(step):
        return pltpu.make_async_remote_copy(
            src_ref=tot,
            dst_ref=tots.at[step - 1],
            send_sem=tot_send,
            recv_sem=tot_recv.at[step - 1],
            device_id={"tm": lax.rem(when + step, times)},
            device_id_type=MESH,
        )

    def send(k):
        def act(within, core):
            for step in STEPS[within, core][k]:
                main(step).start()

        by_kind(inner, when, act)

    @pl.when(z == low)
    def _():
        signal(down, space=me + ROW)

    for k in range(2):
        loads[k].wait()

        @pl.when(inner)
        def _():
            piece(k).start()

    @pl.when(z < rows - 1)
    def _():
        pl.semaphore_wait(up, 1)

    @pl.when(z > 0)
    def _():
        signal(up, space=me - ROW)

    @pl.when(z == high)
    def _():
        pl.semaphore_wait(down, 1)

    @pl.when(z == 0)
    def _():
        ends(across)
        pl.semaphore_wait(across, group)
        for k in range(1, rows):
            signal(go, space=me + k * ROW)

    loads[2].wait()
    pltpu.make_async_copy(arrived, arrived, load_sem.at[3]).wait()
    send(0)
    for a in range(lat):
        tot[a] = jnp.sum(held[a], axis=0, keepdims=True)
    upper(ones)

    @pl.when(z > 0)
    def _():
        pl.semaphore_wait(go, 1)

    for step in range(1, times):
        total(step).start()
    send(1)
    for step in range(1, times):
        total(step).wait_recv()
    for a in range(lat):
        carry = jnp.zeros((1, lon), jnp.float32)
        for step in range(1, times):
            earlier = jnp.where(when >= step, 1.0, 0.0)
            carry = carry + tots[step - 1, a] * earlier
        held[a, 0:1, :] = held[a, 0:1, :] + carry

    def heads(within, core):
        if within:
            piece_head().start()
        for batch in STEPS[within, core][:5]:
            for step in batch:
                head(step).start()

    by_kind(inner, when, heads)
    send(2)
    for k, step in enumerate((LAST, SPLIT)):
        place = columns(flip(me, step, spaces))

        @pl.loop(0, lat)
        def _(a):
            kept[k, a] = held[a, :, place]

    def put(source, k, rows_in):
        @pl.loop(0, rows_in)
        def _(a):
            out_ref[source * lat + a] = prefix(arrived[k, a], ones)

    @pl.loop(0, lat)
    def _(a):
        out_ref[me * lat + a] = prefix(held[a, :, columns(me)], ones)

    def arrivals(within, core):
        steps = STEPS[within, core][5]
        if within:
            main(steps[0]).wait_recv()
            for step in STEPS[within, core][3]:
                main(step).start()
            piece_head().wait_recv()
            for k in range(2):
                piece(k).wait_recv()
            put(flip(me, SPLIT, spaces), SPLIT - 1, early)
        for step in steps:
            head(step).wait_recv()
            if not within or step != steps[0]:
                main(step).wait_recv()
            put(flip(me, step, spaces), step - 1, lat)
            if step == steps[0]:
                for other in STEPS[within, core][4]:
                    main(other).start()
        count = sum(len(batch) for batch in STEPS[within, core][:5])
        blocks = arrived.at[pl.ds(0, count)]
        pltpu.make_async_copy(blocks, blocks, sent).wait()
        if within:
            rows_out = arrived.at[0, pl.ds(0, early)]
            pltpu.make_async_copy(rows_out, rows_out, piece_sent).wait()

    by_kind(inner, when, arrivals)
    pltpu.make_async_copy(tots, tots, tot_send).wait()


def put_away(first_ref, out_ref, token_ref, sem):
    copy = pltpu.make_async_copy(first_ref, out_ref, sem)
    copy.start()
    token_ref[...] = jnp.zeros_like(token_ref)
    copy.wait()


def rest(spaces, lat, parts, token_ref, kept, out_ref, raw, got, ones, sent, received):
    days, block = got.shape[1:]
    me = lax.axis_index("space")
    z = me // ROW
    inner = (z == spaces // ROW // 2 - 1) | (z == spaces // ROW // 2)
    barrier = pltpu.get_barrier_semaphore()

    @pl.when(inner)
    def _():
        for step in (LAST, SPLIT):
            pl.semaphore_signal(
                barrier, inc=1, device_id={"space": flip(me, step, spaces)}, device_id_type=MESH
            )
        upper(ones)
        pl.semaphore_wait(barrier, 2)

    def copy(step, at, size, to, send_sem, recv_sem, into=got):
        peer = flip(me, step, spaces)
        return pltpu.make_async_remote_copy(
            src_ref=kept.at[(LAST, SPLIT).index(step), pl.ds(at, size)],
            dst_ref=into.at[pl.ds(to, size)],
            send_sem=send_sem,
            recv_sem=recv_sem,
            device_id={"space": peer},
            device_id_type=MESH,
        )

    whole = copy(LAST, 0, lat, 0, sent.at[0], received.at[0])
    at, pieces = lat, []
    for k, (start, size) in enumerate(parts[1:-1]):
        pieces.append((at, size, copy(SPLIT, start, size, at, sent.at[1 + k], received.at[1 + k])))
        at += size
    k = len(parts) - 1
    final = copy(SPLIT, *parts[-1], 0, sent.at[k], received.at[k], raw)

    def put(at, size):
        @pl.loop(at, at + size)
        def _(a):
            out_ref[a] = prefix(got[a], ones)

    @pl.when(inner)
    def _():
        whole.start()
        for _, _, piece in pieces:
            piece.start()
        final.start()
        whole.wait_recv()
        put(0, lat)
        for k, (at, size, piece) in enumerate(pieces):
            piece.wait_recv()
            put(at, size)
        whole.wait_send()
        for _, _, piece in pieces:
            piece.wait_send()
        final.wait()


def finish(spaces, lat, parts, all_ref, late_ref, raw_ref, out_ref, done, ones, sem):
    me = lax.axis_index("space")
    z = me // ROW
    inner = (z == spaces // ROW // 2 - 1) | (z == spaces // ROW // 2)
    start, end, last = parts[1][0], *parts[-1]

    def copy(from_ref, step, at, to, size, k):
        place = flip(me, step, spaces) * lat + to
        return pltpu.make_async_copy(
            from_ref.at[pl.ds(at, size)], out_ref.at[pl.ds(place, size)], sem.at[k]
        )

    @pl.when(inner)
    def _():
        copies = [copy(late_ref, LAST, 0, 0, lat, 0), copy(late_ref, SPLIT, lat, start, end - start, 1)]
        for c in copies:
            c.start()
        upper(ones)
        for a in range(last):
            done[a] = prefix(raw_ref[a], ones)
        copies.append(copy(done, SPLIT, 0, end, last, 2))
        copies[-1].start()
        for c in copies:
            c.wait()


def direct(spaces, times, precip):
    days, lat, lon = precip.shape
    parts = parts_of(lat)
    early = parts[0][1]
    late = lat + sum(size for _, size in parts[1:-1])
    last = parts[-1][1]
    block = lon // spaces
    rows = jnp.transpose(precip, (1, 0, 2))
    dma, plain_sem = pltpu.SemaphoreType.DMA, pltpu.SemaphoreType.REGULAR
    vmem, hbm = pl.BlockSpec(memory_space=pltpu.VMEM), pl.BlockSpec(memory_space=pltpu.HBM)

    def shaped(*shape):
        return jax.ShapeDtypeStruct(shape, jnp.float32)

    first, blocks = pl.pallas_call(
        functools.partial(most, spaces, times, lat // sum(PARTS), early),
        out_shape=(shaped(lat * spaces, block, days), shaped(2, lat, days, block)),
        in_specs=[hbm],
        out_specs=(vmem, vmem),
        scratch_shapes=[
            pltpu.VMEM((lat, days, lon), jnp.float32),
            pltpu.VMEM((spaces - 1, lat, days, block), jnp.float32),
            pltpu.VMEM((lat, 1, lon), jnp.float32),
            pltpu.VMEM((times - 1, lat, 1, lon), jnp.float32),
            pltpu.VMEM((days, days), jnp.float32),
            dma((4,)),
            dma,
            dma((spaces - 1,)),
            dma,
            dma((3,)),
            dma((spaces - 1,)),
            dma,
            dma((times - 1,)),
            plain_sem,
            plain_sem,
            plain_sem,
            plain_sem,
        ],
        compiler_params=pltpu.CompilerParams(
            collective_id=0, has_side_effects=True, vmem_limit_bytes=GRANT
        ),
        name="most",
    )(rows)
    whole, token = pl.pallas_call(
        put_away,
        out_shape=(shaped(lat * spaces, block, days), shaped(8, 128)),
        in_specs=[vmem],
        out_specs=(hbm, vmem),
        scratch_shapes=[dma],
        compiler_params=pltpu.CompilerParams(vmem_limit_bytes=GRANT),
        name="put_away",
    )(first)
    more, raw = pl.pallas_call(
        functools.partial(rest, spaces, lat, parts),
        out_shape=(shaped(late, block, days), shaped(last, days, block)),
        in_specs=[vmem, vmem],
        out_specs=(vmem, vmem),
        scratch_shapes=[
            pltpu.VMEM((late, days, block), jnp.float32),
            pltpu.VMEM((days, days), jnp.float32),
            dma((len(parts),)),
            dma((len(parts),)),
        ],
        compiler_params=pltpu.CompilerParams(
            collective_id=1, has_side_effects=True, vmem_limit_bytes=GRANT
        ),
        name="rest",
    )(token, blocks)
    return pl.pallas_call(
        functools.partial(finish, spaces, lat, parts),
        out_shape=shaped(lat * spaces, block, days),
        in_specs=[hbm, vmem, vmem],
        out_specs=hbm,
        input_output_aliases={0: 0},
        scratch_shapes=[
            pltpu.VMEM((last, block, days), jnp.float32),
            pltpu.VMEM((days, days), jnp.float32),
            dma((3,)),
        ],
        compiler_params=pltpu.CompilerParams(vmem_limit_bytes=GRANT),
        name="finish",
    )(whole, more, raw)


def plain(precip):
    days = precip.shape[0]
    position = lax.broadcasted_iota(jnp.int32, (days, days), 0)
    later = lax.broadcasted_iota(jnp.int32, (days, days), 1)
    ones = (position <= later).astype(jnp.float32)
    source = lax.all_to_all(precip, "space", split_axis=2, concat_axis=1, tiled=True)
    pixel_major = jnp.transpose(source, (1, 2, 0))
    running = jnp.dot(
        pixel_major, ones, precision=lax.Precision.HIGHEST, preferred_element_type=jnp.float32
    )
    last = lax.all_gather(running[:, :, -1], "tm")
    place = lax.broadcasted_iota(jnp.int32, last.shape, 0)
    carried = jnp.sum(jnp.where(place < lax.axis_index("tm"), last, 0.0), axis=0)
    return running + carried[:, :, None]


def solution(mesh):
    spaces, times = mesh.shape["space"], mesh.shape["tm"]

    def per_device(precip):
        days, lat, lon = precip.shape
        tiled = lon % (spaces * 128) == 0 and days % 128 == 0
        if tiled and lat % sum(PARTS) == 0 and spaces == SPACES and times > 1 and times % 2 == 0:
            return direct(spaces, times, precip)
        return plain(precip)

    return jax.shard_map(
        per_device,
        mesh=mesh,
        in_specs=(P("tm", "space", None),),
        out_specs=P(None, "space", "tm"),
        check_vma=False,
    )
```
